32 devices in a mesh: dp: 1 (over z), tp: 4 (over y), cp: 8 (over x, core).
Axes of the slice: x: 4, y: 4, z: 1, core: 2. Of those that a mesh axis runs over, the one named last changes fastest.
The devices are a block of a 4x4x8 slice.
Arguments:
- x_tokens: bfloat16 [8192, 5120], P(('dp', 'cp'))
- norm_local: bfloat16 [5120], replicated
- q_local: bfloat16 [5120, 40, 128], P(None, 'tp')
- k_local: bfloat16 [5120, 8, 128], P(None, 'tp')
- v_local: bfloat16 [5120, 8, 128], P(None, 'tp')
- o_local: bfloat16 [40, 128, 5120], P('tp')
- norm_mlp: bfloat16 [5120], replicated
- w_gate: bfloat16 [5120, 16384], P(None, 'tp')
- w_up: bfloat16 [5120, 16384], P(None, 'tp')
- w_down: bfloat16 [16384, 5120], P('tp')
- norm_global: bfloat16 [5120], replicated
- q_global: bfloat16 [5120, 40, 128], P(None, 'tp')
- k_global: bfloat16 [5120, 8, 128], P(None, 'tp')
- v_global: bfloat16 [5120, 8, 128], P(None, 'tp')
- o_global: bfloat16 [40, 128, 5120], P('tp')
Outputs:
- output 1: bfloat16 [8192, 5120], P(('dp', 'cp'))
- output 2: bfloat16 [8192, 8, 128], P(('dp', 'cp'), 'tp')
- output 3: bfloat16 [8192, 8, 128], P(('dp', 'cp'), 'tp')
- output 4: bfloat16 [8192, 8, 128], P(('dp', 'cp'), 'tp')
- output 5: bfloat16 [8192, 8, 128], P(('dp', 'cp'), 'tp')
All inputs are finite; a program needn't handle non-finite values.
Results may differ from the reference program's by a relative error of at most 0.0156764.
Values are sent between devices in bfloat16 or wider.
A program may use at most 768 MiB of HBM per device.

```python
import math
import jax
import jax.numpy as jnp
from jax import lax

SEQ_LEN = 8192
MODEL_DIM = 5120
Q_HEADS = 40
KV_HEADS = 8
HEAD_DIM = 128
FFN_DIM = 16384
LOCAL_CHUNKS = 2
DRIFT_DIMS = 8

CHUNK_LEN = SEQ_LEN // LOCAL_CHUNKS
GROUP_SIZE = Q_HEADS // KV_HEADS
Q_BLOCK = math.gcd(SEQ_LEN, 64)
ROW_BLOCK = math.gcd(SEQ_LEN, 1024)
NORM_EPS = 1e-5
ROPE_THETA = 500000.0
ATTN_SCALE = 0.1


def draw_weight(key, shape, fan_in):
    return (jax.random.normal(key, shape, jnp.float32) * fan_in ** -0.5).astype(jnp.bfloat16)


def draw_gain(key):
    return (1.0 + 0.3 * jax.random.normal(key, (MODEL_DIM,), jnp.float32)).astype(jnp.bfloat16)


def draw_tokens(key):
    walk_key, start_key, dir_key, noise_key = jax.random.split(key, 4)
    moves = jax.random.normal(walk_key, (SEQ_LEN, DRIFT_DIMS), jnp.float32) * SEQ_LEN ** -0.5
    walk = jnp.cumsum(moves, axis=0) + 0.5 * jax.random.normal(start_key, (1, DRIFT_DIMS), jnp.float32)
    directions = jax.random.normal(dir_key, (DRIFT_DIMS, MODEL_DIM), jnp.float32) * DRIFT_DIMS ** -0.5
    noise = jax.random.normal(noise_key, (SEQ_LEN, MODEL_DIM), jnp.float32)
    return (jnp.dot(walk, directions) + 0.5 * noise).astype(jnp.bfloat16)


def setup_inputs(seed: int = 0, part: int = 0) -> dict:
    base_key = jax.random.key(seed)
    keys = jax.random.split(base_key, 14)
    attn_fan = Q_HEADS * HEAD_DIM
    return {
        "x_tokens": draw_tokens(jax.random.fold_in(base_key, part)),
        "norm_local": draw_gain(keys[0]),
        "q_local": draw_weight(keys[1], (MODEL_DIM, Q_HEADS, HEAD_DIM), MODEL_DIM),
        "k_local": draw_weight(keys[2], (MODEL_DIM, KV_HEADS, HEAD_DIM), MODEL_DIM),
        "v_local": draw_weight(keys[3], (MODEL_DIM, KV_HEADS, HEAD_DIM), MODEL_DIM),
        "o_local": draw_weight(keys[4], (Q_HEADS, HEAD_DIM, MODEL_DIM), attn_fan),
        "norm_mlp": draw_gain(keys[5]),
        "w_gate": draw_weight(keys[6], (MODEL_DIM, FFN_DIM), MODEL_DIM),
        "w_up": draw_weight(keys[7], (MODEL_DIM, FFN_DIM), MODEL_DIM),
        "w_down": draw_weight(keys[8], (FFN_DIM, MODEL_DIM), FFN_DIM),
        "norm_global": draw_gain(keys[9]),
        "q_global": draw_weight(keys[10], (MODEL_DIM, Q_HEADS, HEAD_DIM), MODEL_DIM),
        "k_global": draw_weight(keys[11], (MODEL_DIM, KV_HEADS, HEAD_DIM), MODEL_DIM),
        "v_global": draw_weight(keys[12], (MODEL_DIM, KV_HEADS, HEAD_DIM), MODEL_DIM),
        "o_global": draw_weight(keys[13], (Q_HEADS, HEAD_DIM, MODEL_DIM), attn_fan),
    }


def rms_norm(values, gain):
    wide_vals = values.astype(jnp.float32)
    factor = lax.rsqrt(jnp.mean(wide_vals * wide_vals, axis=-1, keepdims=True) + NORM_EPS)
    return (wide_vals * factor * gain.astype(jnp.float32)).astype(jnp.bfloat16)


def head_norm(head_vals):
    factor = lax.rsqrt(jnp.mean(head_vals * head_vals, axis=-1, keepdims=True) + NORM_EPS)
    return head_vals * factor


def rope_tables(positions):
    half = HEAD_DIM // 2
    inv_freq = jnp.power(ROPE_THETA, -(jnp.arange(half, dtype=jnp.float32) * (2.0 / HEAD_DIM)))
    angles = positions.astype(jnp.float32)[:, None] * inv_freq[None, :]
    return jnp.cos(angles), jnp.sin(angles)


def apply_rope(head_vals, cosines, sines):
    half = head_vals.shape[-1] // 2
    pairs = head_vals.reshape(head_vals.shape[:-1] + (half, 2))
    even_part = pairs[..., 0]
    odd_part = pairs[..., 1]
    rotated = jnp.stack([even_part * cosines - odd_part * sines, even_part * sines + odd_part * cosines], axis=-1)
    return rotated.reshape(head_vals.shape)


def project(acts, weight):
    return jnp.einsum("sd,dhe->she", acts.astype(jnp.float32), weight.astype(jnp.float32))


def out_proj(attn, weight):
    return jnp.einsum("she,hed->sd", attn.astype(jnp.float32), weight.astype(jnp.float32))


def attend_block(q_blk, keys, values, q_pos, k_pos):
    rows = q_blk.shape[0]
    q_grp = q_blk.astype(jnp.float32).reshape(rows, KV_HEADS, GROUP_SIZE, HEAD_DIM)
    scores = jnp.einsum("tkge,nke->ktgn", q_grp, keys) * HEAD_DIM ** -0.5
    mask = k_pos[None, :] <= q_pos[:, None]
    scores = jnp.where(mask[None, :, None, :], scores, -jnp.inf)
    peak = jnp.max(scores, axis=-1, keepdims=True)
    weights = jnp.exp(scores - peak)
    denom = jnp.sum(weights, axis=-1)
    numer = jnp.einsum("ktgn,nke->ktge", weights.astype(jnp.bfloat16).astype(jnp.float32), values)
    attn = numer / denom[..., None]
    return jnp.transpose(attn, (1, 0, 2, 3)).reshape(rows, Q_HEADS, HEAD_DIM).astype(jnp.bfloat16)


def local_attention(q_all, k_all, v_all):
    def one_block(block):
        start = block * Q_BLOCK
        chunk_start = (start // CHUNK_LEN) * CHUNK_LEN
        q_blk = lax.dynamic_slice_in_dim(q_all, start, Q_BLOCK, axis=0)
        keys = lax.dynamic_slice_in_dim(k_all, chunk_start, CHUNK_LEN, axis=0)
        values = lax.dynamic_slice_in_dim(v_all, chunk_start, CHUNK_LEN, axis=0)
        return attend_block(q_blk, keys, values, start + jnp.arange(Q_BLOCK), chunk_start + jnp.arange(CHUNK_LEN))

    blocks = lax.map(one_block, jnp.arange(SEQ_LEN // Q_BLOCK))
    return blocks.reshape(SEQ_LEN, Q_HEADS, HEAD_DIM)


def global_attention(q_all, k_all, v_all):
    key_pos = jnp.arange(SEQ_LEN)

    def one_block(block):
        start = block * Q_BLOCK
        q_blk = lax.dynamic_slice_in_dim(q_all, start, Q_BLOCK, axis=0)
        return attend_block(q_blk, k_all, v_all, start + jnp.arange(Q_BLOCK), key_pos)

    blocks = lax.map(one_block, jnp.arange(SEQ_LEN // Q_BLOCK))
    return blocks.reshape(SEQ_LEN, Q_HEADS, HEAD_DIM)


def reference(x_tokens, norm_local, q_local, k_local, v_local, o_local, norm_mlp, w_gate, w_up, w_down, norm_global, q_global, k_global, v_global, o_global):
    positions = jnp.arange(SEQ_LEN)
    cosines, sines = rope_tables(positions)
    cos_heads = cosines[:, None, :]
    sin_heads = sines[:, None, :]
    normed = rms_norm(x_tokens, norm_local)
    q_two = head_norm(apply_rope(project(normed, q_local), cos_heads, sin_heads)).astype(jnp.bfloat16)
    k_two = head_norm(apply_rope(project(normed, k_local), cos_heads, sin_heads)).astype(jnp.bfloat16)
    v_two = project(normed, v_local).astype(jnp.bfloat16)
    attn_two = local_attention(q_two, k_two.astype(jnp.float32), v_two.astype(jnp.float32))
    hidden = (x_tokens.astype(jnp.float32) + out_proj(attn_two, o_local)).astype(jnp.bfloat16)

    def mlp_rows(rows):
        normed_rows = rms_norm(rows, norm_mlp)
        gate_val = jnp.dot(normed_rows, w_gate, preferred_element_type=jnp.float32)
        up_val = jnp.dot(normed_rows, w_up, preferred_element_type=jnp.float32)
        activated = (jax.nn.silu(gate_val) * up_val).astype(jnp.bfloat16)
        down_val = jnp.dot(activated, w_down, preferred_element_type=jnp.float32)
        return (rows.astype(jnp.float32) + down_val).astype(jnp.bfloat16)

    hidden_two = lax.map(mlp_rows, hidden.reshape(SEQ_LEN // ROW_BLOCK, ROW_BLOCK, MODEL_DIM)).reshape(SEQ_LEN, MODEL_DIM)
    normed_three = rms_norm(hidden_two, norm_global)
    temper = jnp.log(((positions + 1) // CHUNK_LEN).astype(jnp.float32) + 1.0) * ATTN_SCALE + 1.0
    q_three = (project(normed_three, q_global) * temper[:, None, None]).astype(jnp.bfloat16)
    k_three = project(normed_three, k_global).astype(jnp.bfloat16)
    v_three = project(normed_three, v_global).astype(jnp.bfloat16)
    attn_three = global_attention(q_three, k_three.astype(jnp.float32), v_three.astype(jnp.float32))
    out_tokens = (hidden_two.astype(jnp.float32) + out_proj(attn_three, o_global)).astype(jnp.bfloat16)
    return (out_tokens, k_two, v_two, k_three, v_three)
```

```python
import functools
import math

import jax
import jax.numpy as jnp
from jax import lax
from jax.experimental import pallas as pl
from jax.experimental.pallas import tpu as pltpu
from jax.sharding import PartitionSpec as P

NORM_EPS = 1e-5
ROPE_THETA = 500000.0
ATTN_SCALE = 0.1
LOCAL_CHUNKS = 2
LANES = 128
CHUNKS = 4
LAG = 2
TILE = 512
WEIGHT_SLOTS = 3
MESH = pl.DeviceIdType.MESH
VMEM_LIMIT = 60 * 1024 * 1024
VMEM_MAX = 67043328
F32 = jnp.float32
BF16 = jnp.bfloat16
MASKED = -1e30


def dot(left, right):
    return lax.dot_general(left, right, (((1,), (0,)), ((), ())), preferred_element_type=F32)


def dot_t(left, right):
    return lax.dot_general(left, right, (((1,), (1,)), ((), ())), preferred_element_type=F32)


def split_kv_kernel(wk_ref, wv_ref, out_ref, wide_ref):
    rows = out_ref.shape[0]
    for part, ref in enumerate((wk_ref, wv_ref)):
        wide_ref[...] = ref[...].astype(F32)
        for head in range(2):
            col = (2 * part + head) * LANES
            out_ref[:, col:col + LANES] = wide_ref[pl.ds(head, rows, stride=2), :].astype(BF16)


def split_kv(w_k, w_v):
    depth, heads, dim = w_k.shape
    block = math.gcd(depth, 1024)
    return pl.pallas_call(
        split_kv_kernel,
        grid=(depth // block,),
        in_specs=[pl.BlockSpec((block * heads, dim), lambda i: (i, 0))] * 2,
        out_specs=pl.BlockSpec((block, 2 * heads * dim), lambda i: (i, 0)),
        out_shape=jax.ShapeDtypeStruct((depth, 2 * heads * dim), BF16),
        scratch_shapes=[pltpu.VMEM((block * heads, dim), F32)],
        compiler_params=pltpu.CompilerParams(vmem_limit_bytes=VMEM_LIMIT),
        cost_estimate=pl.CostEstimate(flops=1000, bytes_accessed=8 * depth * heads * dim, transcendentals=0),
        name="split_kv",
    )(w_k.reshape(depth * heads, dim), w_v.reshape(depth * heads, dim))


def rope_norm(vals, cosines, sines):
    lane = lax.broadcasted_iota(jnp.int32, vals.shape, 1)
    other = jnp.where(lane % 2 == 0, pltpu.roll(vals, LANES - 1, 1), pltpu.roll(vals, 1, 1))
    turned = vals * cosines + other * sines
    return turned * lax.rsqrt(jnp.mean(turned * turned, axis=-1, keepdims=True) + NORM_EPS)


def qkv_kernel(local, sub, *refs):
    if local:
        x_ref, gain_ref, wkv_ref, wq_ref, cos_ref, sin_ref, q_ref, kv_ref, kc_ref, vc_ref, norm_ref, wide_ref = refs
    else:
        x_ref, gain_ref, wkv_ref, wq_ref, temper_ref, q_ref, kv_ref, kc_ref, vc_ref, norm_ref, wide_ref = refs
    step = pl.program_id(0)
    rows = x_ref.shape[0]
    if not local:
        norm_ref = x_ref

    @pl.when((step == 0) & local)
    def _():
        gain = gain_ref[...].astype(F32)
        block = min(rows, 64)

        def norm_rows(i, carry):
            at = pl.ds(pl.multiple_of(i * block, block), block)
            vals = x_ref[at, :].astype(F32)
            factor = lax.rsqrt(jnp.mean(vals * vals, axis=-1, keepdims=True) + NORM_EPS)
            norm_ref[at, :] = (vals * factor * gain).astype(BF16)
            return carry

        lax.fori_loop(0, rows // block, norm_rows, 0)

    @pl.when(step == 0)
    def _():
        for r in range(0, rows, sub):
            at = slice(r, r + sub)
            prod = dot(norm_ref[at, :], wkv_ref[...])
            for head in range(2):
                key = prod[:, head * LANES:(head + 1) * LANES]
                if local:
                    key = rope_norm(key, cos_ref[at, :], sin_ref[at, :])
                kv_ref[0, head, at, :] = key.astype(BF16)
                val = prod[:, (2 + head) * LANES:(3 + head) * LANES]
                for i in range(0, sub, LANES):
                    kv_ref[1, head, r + i:r + i + LANES, :] = val[i:i + LANES].T.astype(BF16)
                wide_ref[pl.ds(2 * r + head, sub, stride=2), :] = key
            kc_ref[2 * r:2 * (r + sub), :] = wide_ref[2 * r:2 * (r + sub), :].astype(BF16)
            for head in range(2):
                val = prod[:, (2 + head) * LANES:(3 + head) * LANES]
                wide_ref[pl.ds(2 * r + head, sub, stride=2), :] = val
            vc_ref[2 * r:2 * (r + sub), :] = wide_ref[2 * r:2 * (r + sub), :].astype(BF16)

    @pl.when(step > 0)
    def _():
        weight = jnp.concatenate([wq_ref[0], wq_ref[1]], axis=1)
        for r in range(0, rows, sub):
            at = slice(r, r + sub)
            prod = dot(norm_ref[at, :], weight)
            for head in range(2):
                query = prod[:, head * LANES:(head + 1) * LANES]
                if local:
                    query = rope_norm(query, cos_ref[at, :], sin_ref[at, :])
                else:
                    query = query * temper_ref[at, :]
                q_ref[head, at, :] = query.astype(BF16)


def qkv(x_rows, gain, w_kv, w_q, tables, local):
    rows, depth = x_rows.shape
    heads = w_q.shape[0]
    whole = lambda shape: pl.BlockSpec(shape, lambda i: (0,) * len(shape))
    prev = lambda i: (jnp.maximum(i - 1, 0), 0, 0)
    return pl.pallas_call(
        functools.partial(qkv_kernel, local, min(rows, 256)),
        grid=(1 + heads // 2,),
        in_specs=[whole((rows, depth)), whole((1, depth)), whole(w_kv.shape), pl.BlockSpec((2, depth, LANES), prev)]
        + [whole((rows, LANES))] * len(tables),
        out_specs=[pl.BlockSpec((2, rows, LANES), prev), whole((2, 2, rows, LANES)), whole((2 * rows, LANES)), whole((2 * rows, LANES))],
        out_shape=[
            jax.ShapeDtypeStruct((heads, rows, LANES), BF16),
            jax.ShapeDtypeStruct((2, 2, rows, LANES), BF16),
            jax.ShapeDtypeStruct((2 * rows, LANES), BF16),
            jax.ShapeDtypeStruct((2 * rows, LANES), BF16),
        ],
        scratch_shapes=[pltpu.VMEM((rows if local else 16, depth), BF16), pltpu.VMEM((2 * rows, LANES), F32)],
        compiler_params=pltpu.CompilerParams(vmem_limit_bytes=VMEM_LIMIT, dimension_semantics=("arbitrary",)),
        cost_estimate=pl.CostEstimate(flops=2 * rows * depth * (heads + 4) * LANES, bytes_accessed=2 * depth * (rows + (heads + 4) * LANES), transcendentals=0),
        name="qkv_local" if local else "qkv_global",
    )(x_rows, gain.reshape(1, depth), w_kv, w_q, *tables)


def flash_kernel(local, factor, step_keys, pos_ref, q_ref, kv_ref, o_ref, peak_ref, denom_ref, numer_ref, qt_ref):
    chunk = pl.program_id(1)
    group, tile, dim = q_ref.shape
    shard_keys = kv_ref.shape[3]
    pos = pos_ref[0]
    denom_ref[...] = jnp.zeros_like(denom_ref)
    numer_ref[...] = jnp.zeros_like(numer_ref)
    if not local:
        peak_ref[...] = jnp.full_like(peak_ref, MASKED)
    for h in range(group):
        qt_ref[h] = q_ref[h].astype(F32).T.astype(BF16)

    def fold(shard, start, count, offset):
        keys = kv_ref[shard, 0, 0, pl.ds(start, count), :]
        vals_t = jnp.concatenate([kv_ref[shard, 1, 0, pl.ds(start + i, dim), :] for i in range(0, count, dim)], axis=1)
        if offset is not None:
            key_idx = lax.broadcasted_iota(jnp.int32, (count, tile), 0) + offset
            visible = key_idx <= lax.broadcasted_iota(jnp.int32, (count, tile), 1)

        def soft(h, scores):
            if local:
                weights = jnp.exp2(scores * factor)
                if offset is not None:
                    weights = jnp.where(visible, weights, 0.0)
                return weights, None
            if offset is not None:
                scores = jnp.where(visible, scores, MASKED)
            old = peak_ref[h]
            high = jnp.maximum(old, jnp.max(scores, axis=0, keepdims=True) * factor)
            peak_ref[h] = high
            return jnp.exp2(scores * factor - high), jnp.exp2(old - high)

        ahead = {}
        for h in range(group + LAG):
            if h < group:
                ahead[h] = dot(keys, qt_ref[h])
            g = h - LAG
            if g >= 0:
                weights, shrink = soft(g, ahead.pop(g))
                sums = jnp.sum(weights.reshape(count // 8, 8, tile), axis=0)
                prod = dot(vals_t, weights.astype(BF16))
                if local:
                    denom_ref[g] += sums
                    numer_ref[g] += prod
                else:
                    denom_ref[g] = denom_ref[g] * shrink + sums
                    numer_ref[g] = numer_ref[g] * shrink + prod

    per_step = step_keys // tile
    if per_step == 1:
        fold(pos, pl.multiple_of(chunk * tile, tile), tile, 0)
    else:
        for r in range(per_step):
            @pl.when(chunk % per_step == r)
            def _():
                fold(pos, pl.multiple_of((chunk - r) * tile, tile), (r + 1) * tile, -r * tile)

    def body(i, carry):
        shard = i // (shard_keys // step_keys)
        fold(shard, pl.multiple_of((i % (shard_keys // step_keys)) * step_keys, step_keys), step_keys, None)
        return carry

    lax.fori_loop(0, pos * (shard_keys // step_keys) + chunk // per_step, body, 0)
    for h in range(group):
        total = jnp.sum(denom_ref[h], axis=0, keepdims=True)
        o_ref[:, h * dim:(h + 1) * dim] = (numer_ref[h] * (1.0 / total)).T.astype(BF16)


def flash(q, kv_all, pos, local, tile, scale):
    heads, tokens, dim = q.shape
    shards, _, kv_heads, _, _ = kv_all.shape
    group = heads // kv_heads
    step_keys = min(tokens, 2 * tile)
    kernel = functools.partial(flash_kernel, local, scale * math.log2(math.e), step_keys)
    pairs = heads * tokens * tokens * shards // 2
    return pl.pallas_call(
        kernel,
        grid_spec=pltpu.PrefetchScalarGridSpec(
            num_scalar_prefetch=1,
            grid=(kv_heads, tokens // tile),
            in_specs=[
                pl.BlockSpec((group, tile, dim), lambda g, c, p: (g, c, 0)),
                pl.BlockSpec((shards, 2, 1, tokens, dim), lambda g, c, p: (0, 0, g, 0, 0)),
            ],
            out_specs=pl.BlockSpec((tile, group * dim), lambda g, c, p: (c, g)),
            scratch_shapes=[pltpu.VMEM((group, 1, tile), F32), pltpu.VMEM((group, 8, tile), F32), pltpu.VMEM((group, dim, tile), F32), pltpu.VMEM((group, dim, tile), BF16)],
        ),
        out_shape=jax.ShapeDtypeStruct((tokens, heads * dim), BF16),
        compiler_params=pltpu.CompilerParams(vmem_limit_bytes=VMEM_LIMIT, dimension_semantics=("arbitrary", "arbitrary")),
        cost_estimate=pl.CostEstimate(flops=8 * pairs * dim, bytes_accessed=4 * shards * kv_heads * tokens * dim, transcendentals=pairs),
        name="flash_local" if local else "flash_global",
    )(pos, q, kv_all)
class Exchange:
    def __init__(self, part, near, far, gath, send_sems, recv_sems):
        self.part, self.near, self.far, self.gath = part, near, far, gath
        self.send_sems, self.recv_sems = send_sems, recv_sems
        self.me = lax.axis_index("tp")
        self.right, self.opposite, self.left = (lax.rem(self.me + i, 4) for i in (1, 2, 3))
        self.quarter = part.shape[1] // 4
        self.width = part.shape[2]
        self.low, self.high = pl.ds(0, self.width // 2), pl.ds(self.width // 2, self.width // 2)
        self.all = pl.ds(0, self.width)

    def barrier(self):
        sem = pltpu.get_barrier_semaphore()
        for device in (self.left, self.right):
            pl.semaphore_signal(sem, inc=1, device_id={"tp": device}, device_id_type=MESH)
        pl.semaphore_wait(sem, 2)

    def rows(self, owner):
        return pl.ds(pl.multiple_of(owner * self.quarter, self.quarter), self.quarter)

    def copies(self, name, stage, c):
        kind = ("near", "early", "late", "own", "pass").index(name)
        pairs = {
            "near": ((self.opposite, self.low), (self.opposite, self.high)),
            "early": ((self.right, self.high), (self.left, self.low)),
            "late": ((self.right, self.low), (self.left, self.high)),
            "own": ((self.me, self.all), (self.me, self.all)),
            "pass": ((self.left, self.low), (self.right, self.high)),
        }[name]
        made = []
        for way, (owner, cols) in enumerate(pairs):
            if name in ("own", "pass"):
                source = self.gath.at[c, self.rows(owner), cols]
                target = self.gath.at[c, self.rows(owner), cols]
            else:
                source = self.part.at[c, self.rows(owner), cols]
                target = self.near.at[c, way] if name == "near" else self.far.at[c, way, pl.ds(0, self.quarter), cols]
            made.append(pltpu.make_async_remote_copy(
                src_ref=source, dst_ref=target,
                send_sem=self.send_sems.at[stage, kind, way, c], recv_sem=self.recv_sems.at[stage, kind, way, c],
                device_id={"tp": (self.right, self.left)[way]}, device_id_type=MESH))
        return made

    def start(self, name, stage, c):
        for copy in self.copies(name, stage, c):
            copy.start()

    def wait_sent(self, stage, c):
        for name in ("near", "early", "late", "own", "pass"):
            for copy in self.copies(name, stage, c):
                copy.wait_send()

    def arrived(self, name, stage, c):
        for copy in self.copies(name, stage, c):
            copy.wait_recv()

    def begin(self, stage, c):
        self.start("near", stage, c)
        self.start("early", stage, c)

    def relay(self, stage, c):
        self.arrived("near", stage, c)
        half = self.width // 2
        for way, (owner, first) in enumerate(((self.right, 0), (self.left, half))):
            def add(i, carry, way=way, owner=owner, first=first):
                at = pl.ds(pl.multiple_of(owner * self.quarter + i * 16, 16), 16)
                cols = pl.ds(first, half)
                mine = self.part[c, at, cols].astype(F32)
                self.part[c, at, cols] = (mine + self.near[c, way, pl.ds(pl.multiple_of(i * 16, 16), 16), :].astype(F32)).astype(BF16)
                return carry

            lax.fori_loop(0, self.quarter // 16, add, 0)
        self.start("late", stage, c)

    def finish(self, stage, c, base, gain):
        self.arrived("early", stage, c)
        self.arrived("late", stage, c)

        def total(i, carry):
            at = pl.ds(pl.multiple_of(i * 16, 16), 16)
            mine = pl.ds(pl.multiple_of(self.me * self.quarter + i * 16, 16), 16)
            sums = self.part[c, mine, :].astype(F32) + self.far[c, 0, at, :].astype(F32) + self.far[c, 1, at, :].astype(F32)
            vals = (base[c, at, :].astype(F32) + sums).astype(BF16)
            base[c, at, :] = vals
            if gain is None:
                self.gath[c, mine, :] = vals
            else:
                wide = vals.astype(F32)
                factor = lax.rsqrt(jnp.mean(wide * wide, axis=-1, keepdims=True) + NORM_EPS)
                self.gath[c, mine, :] = (wide * factor * gain[...].astype(F32)).astype(BF16)
            return carry

        lax.fori_loop(0, self.quarter // 16, total, 0)
        self.start("own", stage, c)

    def forward(self, stage, c):
        self.arrived("own", stage, c)
        self.start("pass", stage, c)

    def done(self, stage, c):
        self.arrived("pass", stage, c)


def project_out(exchange, attn_ref, w_out_ref, attn_buf, attn_sem, wbuf, wsem, run_between):
    depth, width = w_out_ref.shape
    per_slot = wbuf.shape[1] // depth
    tiles = width // TILE
    rows = attn_buf.shape[1]

    def tile(k):
        return wbuf.at[k // per_slot, pl.ds(pl.multiple_of(lax.rem(k, per_slot) * depth, depth), depth)]

    def load(k):
        return pltpu.make_async_copy(w_out_ref.at[:, pl.ds(pl.multiple_of(k * TILE, TILE), TILE)], tile(k), wsem.at[k])

    def attn(c):
        return pltpu.make_async_copy(attn_ref.at[pl.ds(c * rows, rows)], attn_buf.at[c], attn_sem.at[c])

    for c in range(CHUNKS):
        attn(c).start()
    for k in range(tiles):
        load(k).start()
    exchange.barrier()
    for c in range(CHUNKS):
        attn(c).wait()

        def step(k, carry, c=c):
            if c == 0:
                load(k).wait()
            exchange.part[c, :, pl.ds(pl.multiple_of(k * TILE, TILE), TILE)] = dot(attn_buf[c], tile(k)[...]).astype(BF16)
            return carry

        lax.fori_loop(0, tiles, step, 0)
        exchange.begin(0, c)
        run_between(c)


def early_steps(exchange, base, gain):
    relay = lambda c: exchange.relay(0, c)
    finish = lambda c: exchange.finish(0, c, base, gain)
    forward = lambda c: exchange.forward(0, c)

    def between(c):
        if c >= 1:
            relay(c - 1)
        if c >= 2:
            finish(c - 2)
        if c >= 3:
            forward(c - 3)

    return between


def mlp_kernel(attn_ref, w_out_ref, x_ref, gain_mlp, gain_next, w_gate, w_up, w_down, h_ref, n_ref,
               part, near, far, gath, base, attn_buf, wbuf, act, send_sems, recv_sems, attn_sem, base_sem, wsem, tsem, out_sem):
    ex = Exchange(part, near, far, gath, send_sems, recv_sems)
    rows, width = part.shape[1:]
    depth = w_down.shape[0]
    half = TILE // 2
    ups, downs = depth // half, width // TILE
    tiles = ups + downs
    me = ex.me

    def base_copy(c):
        return pltpu.make_async_copy(x_ref.at[pl.ds(pl.multiple_of(c * rows + me * ex.quarter, ex.quarter), ex.quarter)], base.at[c], base_sem.at[c])

    for c in range(CHUNKS):
        base_copy(c).start()

    def between(c):
        if c == 0:
            for k in range(CHUNKS):
                base_copy(k).wait()
        early_steps(ex, base, gain_mlp)(c)

    project_out(ex, attn_ref, w_out_ref, attn_buf, attn_sem, wbuf, wsem, between)

    def up_copies(s, slot):
        cols = pl.ds(pl.multiple_of(s * half, half), half)
        return (pltpu.make_async_copy(w_gate.at[:, cols], wbuf.at[slot, :, pl.ds(0, half)], tsem.at[slot, 0]),
                pltpu.make_async_copy(w_up.at[:, cols], wbuf.at[slot, :, pl.ds(half, half)], tsem.at[slot, 1]))

    def down_copy(s, slot):
        return pltpu.make_async_copy(w_down.at[:, pl.ds(pl.multiple_of(s * TILE, TILE), TILE)], wbuf.at[slot, pl.ds(0, depth)], tsem.at[slot, 0])

    def fetch(s, slot):
        @pl.when(s < ups)
        def _():
            for copy in up_copies(s, slot):
                copy.start()

        @pl.when(s >= ups)
        def _():
            down_copy(s - ups, slot).start()

    ahead = WEIGHT_SLOTS - 1
    for t in range(ahead):
        for copy in up_copies(t, t):
            copy.start()
    first = {0: [(0.04, lambda: ex.finish(0, 2, base, gain_mlp)), (0.12, lambda: ex.relay(0, 3)), (0.2, lambda: ex.forward(0, 1)),
                 (0.31, lambda: ex.finish(0, 3, base, gain_mlp)), (0.43, lambda: ex.forward(0, 2)), (0.62, lambda: ex.forward(0, 3))]}
    ex.done(0, 0)
    for c in range(CHUNKS):
        actions = list(first.get(c, []))
        if c >= 1:
            p = c - 1
            actions += [(0.2, lambda p=p: ex.relay(1, p)), (0.43, lambda p=p: ex.finish(1, p, base, gain_next)), (0.77, lambda p=p: ex.forward(1, p))]
        if c >= 2:
            p = c - 2
            actions += [(0.12, lambda p=p: leave(p))]

        def leave(p):
            ex.done(1, p)
            pltpu.make_async_copy(gath.at[p], n_ref.at[pl.ds(p * rows, rows)], out_sem.at[p, 0]).start()
            pltpu.make_async_copy(base.at[p], h_ref.at[p], out_sem.at[p, 1]).start()

        def serve(s, actions=actions):
            for at, action in actions:
                pl.when(s == int(at * tiles))(action)

        def refill(s, t):
            nxt = s + ahead
            if c + 1 < CHUNKS:
                fetch(lax.rem(nxt, tiles), lax.rem(t + ahead, WEIGHT_SLOTS))
            else:
                pl.when(nxt < tiles)(lambda: fetch(nxt, lax.rem(t + ahead, WEIGHT_SLOTS)))

        def up_step(s, carry, c=c):
            t = c * tiles + s
            slot = lax.rem(t, WEIGHT_SLOTS)
            for copy in up_copies(s, slot):
                copy.wait()
            refill(s, t)
            prod = dot(gath[c], wbuf[slot])
            gate = prod[:, :half]
            act[:, pl.ds(pl.multiple_of(s * half, half), half)] = (gate / (1.0 + jnp.exp(-gate)) * prod[:, half:]).astype(BF16)
            serve(s)
            return carry

        def down_step(s, carry, c=c):
            t = c * tiles + ups + s
            slot = lax.rem(t, WEIGHT_SLOTS)
            down_copy(s, slot).wait()
            refill(ups + s, t)
            part[c, :, pl.ds(pl.multiple_of(s * TILE, TILE), TILE)] = dot(act[...], wbuf[slot, pl.ds(0, depth)]).astype(BF16)
            serve(ups + s)
            return carry

        lax.fori_loop(0, ups, up_step, 0)
        ex.wait_sent(0, c)
        lax.fori_loop(0, downs, down_step, 0)
        ex.begin(1, c)
        if c + 1 < CHUNKS:
            ex.done(0, c + 1)
    last = CHUNKS - 1
    ex.relay(1, last)
    leave(last - 1)
    ex.finish(1, last, base, gain_next)
    ex.forward(1, last)
    leave(last)
    for c in range(CHUNKS):
        ex.wait_sent(1, c)
        pltpu.make_async_copy(gath.at[c], n_ref.at[pl.ds(c * rows, rows)], out_sem.at[c, 0]).wait()
        pltpu.make_async_copy(base.at[c], h_ref.at[c], out_sem.at[c, 1]).wait()


def exchange_scratch(rows, width, stages):
    quarter = rows // 4
    return [
        pltpu.VMEM((CHUNKS, rows, width), BF16),
        pltpu.VMEM((CHUNKS, 2, quarter, width // 2), BF16),
        pltpu.VMEM((CHUNKS, 2, quarter, width), BF16),
        pltpu.VMEM((CHUNKS, rows, width), BF16),
        pltpu.VMEM((CHUNKS, quarter, width), BF16),
    ]


ANY = pl.BlockSpec(memory_space=pl.ANY)
IN_VMEM = pl.BlockSpec(memory_space=pltpu.VMEM)


def mlp_block(attn, w_out, x_tokens, gain_mlp, gain_next, w_gate, w_up, w_down):
    tokens, width = x_tokens.shape
    rows = tokens // CHUNKS
    depth = w_down.shape[0]
    slot_rows = max(width, depth)
    flops = 2 * tokens * width * (w_out.shape[0] + 3 * depth)
    return pl.pallas_call(
        mlp_kernel,
        in_specs=[ANY, ANY, ANY, IN_VMEM, IN_VMEM, ANY, ANY, ANY],
        out_specs=[ANY, ANY],
        out_shape=[jax.ShapeDtypeStruct((CHUNKS, rows // 4, width), BF16), jax.ShapeDtypeStruct((tokens, width), BF16)],
        scratch_shapes=exchange_scratch(rows, width, 2) + [
            pltpu.VMEM((CHUNKS, rows, w_out.shape[0]), BF16),
            pltpu.VMEM((WEIGHT_SLOTS, slot_rows, TILE), BF16),
            pltpu.VMEM((rows, depth), BF16),
            pltpu.SemaphoreType.DMA((2, 5, 2, CHUNKS)),
            pltpu.SemaphoreType.DMA((2, 5, 2, CHUNKS)),
            pltpu.SemaphoreType.DMA((CHUNKS,)),
            pltpu.SemaphoreType.DMA((CHUNKS,)),
            pltpu.SemaphoreType.DMA((width // TILE,)),
            pltpu.SemaphoreType.DMA((WEIGHT_SLOTS, 2)),
            pltpu.SemaphoreType.DMA((CHUNKS, 2)),
        ],
        compiler_params=pltpu.CompilerParams(vmem_limit_bytes=VMEM_MAX, collective_id=1, has_side_effects=True),
        cost_estimate=pl.CostEstimate(flops=flops, bytes_accessed=8 * depth * width * CHUNKS, transcendentals=0),
        name="mlp_block",
    )(attn, w_out, x_tokens, gain_mlp.reshape(1, width), gain_next.reshape(1, width), w_gate, w_up, w_down)


def out_kernel(attn_ref, w_out_ref, h_ref, out_ref, part, near, far, gath, base, attn_buf, wbuf,
               send_sems, recv_sems, attn_sem, base_sem, wsem, out_sem):
    ex = Exchange(part, near, far, gath, send_sems, recv_sems)
    rows = part.shape[1]

    def base_copy(c):
        return pltpu.make_async_copy(h_ref.at[c], base.at[c], base_sem.at[c])

    def leave(c):
        ex.done(0, c)
        pltpu.make_async_copy(gath.at[c], out_ref.at[pl.ds(c * rows, rows)], out_sem.at[c]).start()

    for c in range(CHUNKS):
        base_copy(c).start()

    def between(c):
        if c == 0:
            for k in range(CHUNKS):
                base_copy(k).wait()
        early_steps(ex, base, None)(c)

    project_out(ex, attn_ref, w_out_ref, attn_buf, attn_sem, wbuf, wsem, between)
    last = CHUNKS - 1
    ex.finish(0, last - 1, base, None)
    ex.relay(0, last)
    leave(0)
    ex.forward(0, last - 2)
    ex.finish(0, last, base, None)
    ex.forward(0, last - 1)
    leave(1)
    ex.forward(0, last)
    leave(2)
    leave(3)
    for c in range(CHUNKS):
        ex.wait_sent(0, c)
        pltpu.make_async_copy(gath.at[c], out_ref.at[pl.ds(c * rows, rows)], out_sem.at[c]).wait()


def out_block(attn, w_out, hidden):
    tokens, depth = attn.shape
    width = w_out.shape[1]
    rows = tokens // CHUNKS
    per_slot = max(1, width // depth)
    return pl.pallas_call(
        out_kernel,
        in_specs=[ANY, ANY, ANY],
        out_specs=ANY,
        out_shape=jax.ShapeDtypeStruct((tokens, width), BF16),
        scratch_shapes=exchange_scratch(rows, width, 1) + [
            pltpu.VMEM((CHUNKS, rows, depth), BF16),
            pltpu.VMEM((pl.cdiv(width // TILE, per_slot), per_slot * depth, TILE), BF16),
            pltpu.SemaphoreType.DMA((1, 5, 2, CHUNKS)),
            pltpu.SemaphoreType.DMA((1, 5, 2, CHUNKS)),
            pltpu.SemaphoreType.DMA((CHUNKS,)),
            pltpu.SemaphoreType.DMA((CHUNKS,)),
            pltpu.SemaphoreType.DMA((width // TILE,)),
            pltpu.SemaphoreType.DMA((CHUNKS,)),
        ],
        compiler_params=pltpu.CompilerParams(vmem_limit_bytes=VMEM_MAX, collective_id=2, has_side_effects=True),
        cost_estimate=pl.CostEstimate(flops=2 * tokens * width * depth, bytes_accessed=4 * depth * width, transcendentals=0),
        name="out_block",
    )(attn, w_out, hidden)


def solution(mesh):
    cp_size = mesh.shape["cp"]
    chunk_shards = cp_size // LOCAL_CHUNKS
    local_groups = [list(range(g * chunk_shards, (g + 1) * chunk_shards)) for g in range(LOCAL_CHUNKS)]

    def shard_body(x_tokens, norm_local, q_local, k_local, v_local, o_local, norm_mlp, w_gate, w_up, w_down, norm_global, q_global, k_global, v_global, o_global):
        tokens, model_dim = x_tokens.shape
        head_dim = k_local.shape[2]
        chunk_len = tokens * cp_size // LOCAL_CHUNKS
        scale = head_dim ** -0.5
        shard_idx = lax.axis_index("cp")
        positions = shard_idx * tokens + jnp.arange(tokens)
        half = jnp.arange(head_dim) // 2
        inv_freq = jnp.power(ROPE_THETA, -(half.astype(F32) * (2.0 / head_dim)))
        angles = positions.astype(F32)[:, None] * inv_freq[None, :]
        cosines = jnp.cos(angles)
        sines = jnp.sin(angles) * jnp.where(jnp.arange(head_dim) % 2 == 0, -1.0, 1.0)
        rows = tokens // CHUNKS

        w_kv_local = split_kv(k_local, v_local)
        w_kv_global = split_kv(k_global, v_global)
        o_two = o_local.reshape(-1, model_dim)
        o_three = o_global.reshape(-1, model_dim)

        q_two, kv_two, kc_two, vc_two = qkv(x_tokens, norm_local, w_kv_local, jnp.transpose(q_local, (1, 0, 2)), (cosines, sines), True)
        kv_all = lax.all_gather(kv_two, "cp", axis_index_groups=local_groups)
        attn_two = flash(q_two, kv_all, (shard_idx % chunk_shards).astype(jnp.int32).reshape(1), True, rows, scale)
        hidden_two, normed_three = mlp_block(attn_two, o_two, x_tokens, norm_mlp, norm_global, w_gate, w_up, w_down)

        temper = jnp.log(((positions + 1) // chunk_len).astype(F32) + 1.0) * ATTN_SCALE + 1.0
        temper = jnp.broadcast_to(temper[:, None], (tokens, head_dim))
        q_three, kv_three, kc_three, vc_three = qkv(normed_three, norm_global, w_kv_global, jnp.transpose(q_global, (1, 0, 2)), (temper,), False)
        kv_all = lax.all_gather(kv_three, "cp")
        attn_three = flash(q_three, kv_all, shard_idx.astype(jnp.int32).reshape(1), False, rows, scale)
        out_tokens = out_block(attn_three, o_three, hidden_two)
        cache = lambda interleaved: interleaved.reshape(tokens, 2, head_dim)
        return out_tokens, cache(kc_two), cache(vc_two), cache(kc_three), cache(vc_three)

    row_spec = P(("dp", "cp"), None)
    cache_spec = P(("dp", "cp"), "tp", None)
    gain_spec = P(None)
    head_spec = P(None, "tp", None)
    out_spec = P("tp", None, None)
    col_spec = P(None, "tp")
    down_spec = P("tp", None)
    in_specs = (row_spec, gain_spec, head_spec, head_spec, head_spec, out_spec, gain_spec, col_spec, col_spec, down_spec, gain_spec, head_spec, head_spec, head_spec, out_spec)
    out_specs = (row_spec, cache_spec, cache_spec, cache_spec, cache_spec)
    return jax.shard_map(shard_body, mesh=mesh, in_specs=in_specs, out_specs=out_specs, check_vma=False)
```
